128 devices in a mesh: rep: 2 (over core), dp: 64 (over x, y, z).
Axes of the slice: x: 4, y: 4, z: 4, core: 2. Of those that a mesh axis runs over, the one named last changes fastest.
Arguments:
- a: bfloat16 [128, 2, 4096, 1024], P(('rep', 'dp')), parts along dimension 0
- g: bfloat16 [128, 2, 4096, 3328], P(('rep', 'dp')), parts along dimension 0
Outputs:
- output: bfloat16 [4, 1024, 3328], P('rep'), parts along dimension 0
There are 2 independent parts. The reference program is written for one: setup_inputs(seed, part) draws one part's arguments, and reference() takes and returns one part's arrays. A program takes and returns all parts, laid end to end along the dimension named above; each array names one.
All inputs are finite; a program needn't handle non-finite values.
Results may differ from the reference program's by a relative error of at most 0.012.
Values are sent between devices in bfloat16 or wider.
A program may use at most 1.5 GiB of HBM per device.

```python
import jax
import jax.numpy as jnp
from jax import lax

DEVICES = 64
MATRICES = 2
TOKENS = 4096
D = 1024
FF = 3328


def setup_inputs(seed: int = 0, part: int = 0) -> dict:
    ka, kg, ks = (jax.random.fold_in(k, part) for k in jax.random.split(jax.random.key(seed), 3))
    size = 2.0 ** jax.random.uniform(ks, (DEVICES, MATRICES, 1, 1), jnp.float32, -1.0, 1.0)
    a = jax.random.normal(ka, (DEVICES, MATRICES, TOKENS, D), jnp.float32)
    g = size * jax.random.normal(kg, (DEVICES, MATRICES, TOKENS, FF), jnp.float32) * (DEVICES * TOKENS) ** -0.5
    return {"a": a.astype(jnp.bfloat16), "g": g.astype(jnp.bfloat16)}


def reference(a, g):
    def take(so_far, one):
        term = jnp.einsum("ntd,ntf->ndf", *one, preferred_element_type=jnp.float32).astype(jnp.bfloat16)
        return so_far + term.astype(jnp.float32), None

    return lax.scan(take, jnp.zeros((MATRICES, D, FF), jnp.float32), (a, g))[0].astype(jnp.bfloat16)
```

```python
import jax
import jax.numpy as jnp
from jax import lax
from jax.experimental import pallas as pl
from jax.experimental.pallas import tpu as pltpu
from jax.sharding import PartitionSpec as P

MESH = pl.DeviceIdType.MESH
F32, BF16 = jnp.float32, jnp.bfloat16
WIDTH = 256
LANES = 128
SLOTS = 6
SIDE = 4
STRIDE = (16, 4, 1)
CHUNK = (256, 64, 16)
TOKENS_AT_ONCE = 512
ROWS_AT_ONCE = 512

OFFSET = (1, 3, 5, 6, 7, 8, 9, 10, 11, 12, 13, 15, 17)


def kernel(
    a_hbm, g_hbm, out_hbm,
    a_in, a_t, g_in, tb0, tb1, tb2, tf1, tf2, mid0, mid1, mid2, got0, got1, got2, sums,
    a_sem, g_sem, o_sem, rs_send, rs_recv, ag_send, ag_recv,
):
    matrices, tokens, rows = a_hbm.shape[1], a_hbm.shape[2], a_hbm.shape[3]
    per_matrix = g_hbm.shape[3] // WIDTH
    units = matrices * per_matrix
    parts = tokens // TOKENS_AT_ONCE

    rep, me = lax.axis_index("rep"), lax.axis_index("dp")
    pos = tuple(lax.rem(me // s, SIDE) for s in STRIDE)

    def neighbour(axis, step):
        return me + (lax.rem(pos[axis] + step + SIDE, SIDE) - pos[axis]) * STRIDE[axis]

    right = tuple(neighbour(axis, 1) for axis in range(3))
    left = tuple(neighbour(axis, -1) for axis in range(3))

    tb, tf, mid, got = (tb0, tb1, tb2), (None, tf1, tf2), (mid0, mid1, mid2), (got0, got1, got2)

    def span(block, size):
        return pl.ds(pl.multiple_of(block * size, size), size)

    def put(src, dst, send, recv, device):
        return pltpu.make_async_remote_copy(
            src_ref=src, dst_ref=dst, send_sem=send, recv_sem=recv, device_id=(rep, device), device_id_type=MESH
        )

    def rs_put(src, u, c, p, kind, way):
        slot = lax.rem(u, SLOTS)
        device = (right, left)[way][(c + p) % 3]
        return put(
            src, got[p].at[u, kind, way], rs_send.at[slot, p, kind, way], rs_recv.at[u, p, kind, way], device
        )

    def rs_first(u, c, p):
        i, own = pos[(c + p) % 3], tb[p].at[lax.rem(u, SLOTS)]
        after, over, before = (span(lax.rem(i + k, SIDE), CHUNK[p]) for k in (1, 2, 3))
        return (
            rs_put(own.at[1, over], u, c, p, 0, 0),
            rs_put(own.at[0, over], u, c, p, 0, 1),
            rs_put(own.at[0, after], u, c, p, 1, 0),
            rs_put(own.at[1, before], u, c, p, 1, 1),
        )

    def rs_second(u, c, p):
        slot = lax.rem(u, SLOTS)
        return tuple(rs_put(mid[p].at[slot, way], u, c, p, 2, way) for way in (0, 1))

    def own_term(u, p, half, block):
        own = (tb[0] if p == 0 else tf[p])[lax.rem(u, SLOTS), half, span(block, CHUNK[p])]
        return own.astype(F32)

    def rs_middle(u, c, p):
        i, slot = pos[(c + p) % 3], lax.rem(u, SLOTS)
        copies = rs_first(u, c, p)
        for copy in copies[:2]:
            copy.wait_recv()
        for copy in copies:
            copy.wait_send()
        for way, half, step in ((0, 1, 1), (1, 0, 3)):
            total = own_term(u, p, half, lax.rem(i + step, SIDE)) + got[p][u, 0, way].astype(F32)
            mid[p][slot, way] = total.astype(BF16)

    def block_rows(c, p):
        first = 0
        for q in range(p):
            first = first + pos[(c + q) % 3] * CHUNK[q]
        return first

    def blk(c, p, step):
        first = block_rows(c, p) + lax.rem(pos[(c + p) % 3] + step, SIDE) * CHUNK[p]
        return pl.ds(pl.multiple_of(first, CHUNK[p]), CHUNK[p])

    def rs_end(u, c, p):
        i, slot = pos[(c + p) % 3], lax.rem(u, SLOTS)
        for copy in rs_first(u, c, p)[2:]:
            copy.wait_recv()
        for copy in rs_second(u, c, p):
            copy.wait_recv()
            copy.wait_send()
        for half in (0, 1):
            total = own_term(u, p, half, i) + got[p][u, 1, half].astype(F32) + got[p][u, 2, 1 - half].astype(F32)
            if p < 2:
                tf[p + 1][slot, half] = total
                tb[p + 1][slot, half] = total.astype(BF16)
            else:
                sums[u, half, blk(c, p, 0)] = total.astype(BF16)

    def ag_put(ref, u, c, p, step, way):
        slot = lax.rem(u, SLOTS)
        device = (right, left)[way][(c + p) % 3]
        return put(ref, ref, ag_send.at[slot, p, step, way], ag_recv.at[u, p, step, way], device)

    def ag_first(u, c, p):
        return tuple(ag_put(sums.at[u, :, blk(c, p, 0)], u, c, p, 0, way) for way in (0, 1))

    def ag_second(u, c, p):
        return (
            ag_put(sums.at[u, 0, blk(c, p, 3)], u, c, p, 1, 0),
            ag_put(sums.at[u, 1, blk(c, p, 1)], u, c, p, 1, 1),
        )

    def start(copies):
        for copy in copies:
            copy.start()

    def wait(copies):
        for copy in copies:
            copy.wait_recv()
            copy.wait_send()

    def out_copies(u):
        n, j = u // per_matrix, lax.rem(u, per_matrix)
        return tuple(
            pltpu.make_async_copy(
                sums.at[u, half],
                out_hbm.at[n, :, pl.ds(pl.multiple_of(j * WIDTH + half * LANES, LANES), LANES)],
                o_sem.at[u, half],
            )
            for half in (0, 1)
        )

    stages = (
        (lambda u, c: None, lambda u, c: start(rs_first(u, c, 0))),
        (lambda u, c: rs_middle(u, c, 0), lambda u, c: start(rs_second(u, c, 0))),
        (lambda u, c: rs_end(u, c, 0), lambda u, c: start(rs_first(u, c, 1))),
        (lambda u, c: rs_middle(u, c, 1), lambda u, c: start(rs_second(u, c, 1))),
        (lambda u, c: rs_end(u, c, 1), lambda u, c: start(rs_first(u, c, 2))),
        (lambda u, c: rs_middle(u, c, 2), lambda u, c: start(rs_second(u, c, 2))),
        (lambda u, c: rs_end(u, c, 2), lambda u, c: start(ag_first(u, c, 2))),
        (lambda u, c: wait(ag_first(u, c, 2)), lambda u, c: start(ag_second(u, c, 2))),
        (lambda u, c: wait(ag_second(u, c, 2)), lambda u, c: start(ag_first(u, c, 1))),
        (lambda u, c: wait(ag_first(u, c, 1)), lambda u, c: start(ag_second(u, c, 1))),
        (lambda u, c: wait(ag_second(u, c, 1)), lambda u, c: start(ag_first(u, c, 0))),
        (lambda u, c: wait(ag_first(u, c, 0)), lambda u, c: start(ag_second(u, c, 0))),
        (lambda u, c: wait(ag_second(u, c, 0)), lambda u, c: start(out_copies(u))),
    )

    def a_copy(n, part):
        return pltpu.make_async_copy(
            a_hbm.at[0, n, span(part, TOKENS_AT_ONCE)], a_in.at[part], a_sem.at[part]
        )

    def g_copy(u):
        n, j, slot = u // per_matrix, lax.rem(u, per_matrix), lax.rem(u, 2)
        return pltpu.make_async_copy(g_hbm.at[0, n, :, span(j, WIDTH)], g_in.at[slot], g_sem.at[slot])

    def load_a(n):
        def one(part, _):
            a_copy(n, part).wait()
            for column in range(0, rows, 256):
                block = a_in[part, :, column : column + 256]
                a_t[column : column + 256, span(part, TOKENS_AT_ONCE)] = block.T
            return 0

        lax.fori_loop(0, parts, one, 0)

    def fetch_a(n):
        def one(part, _):
            a_copy(n, part).start()
            return 0

        lax.fori_loop(0, parts, one, 0)

    def multiply(u):
        g_copy(u).wait()

        @pl.when(u + 1 < units)
        def _():
            g_copy(u + 1).start()

        def one(m, _):
            at = span(m, ROWS_AT_ONCE)
            term = jnp.dot(a_t[at, :], g_in[lax.rem(u, 2)], preferred_element_type=F32).astype(BF16)
            for half in (0, 1):
                tb0[lax.rem(u, SLOTS), half, at] = term[:, half * LANES : (half + 1) * LANES]
            return 0

        lax.fori_loop(0, rows // ROWS_AT_ONCE, one, 0)

    fetch_a(0)
    g_copy(0).start()

    barrier = pltpu.get_barrier_semaphore()
    for device in right + left:
        pl.semaphore_signal(barrier, inc=1, device_id=(rep, device), device_id_type=MESH)
    pl.semaphore_wait(barrier, 6)

    ticks = units + OFFSET[-1]

    def three(group, _):
        for s in range(3):
            t = group * 3 + s
            later = None

            def stage(k, which):
                u, c = t - OFFSET[k], (s - OFFSET[k]) % 3

                @pl.when(jnp.logical_and(u >= 0, u < units))
                def _():
                    stages[k][which](u, c)

            for k in range(len(stages)):
                stage(k, 0)
                if later is not None:
                    stage(later, 1)
                later = k
            stage(later, 1)

            for n in range(matrices):
                if (n * per_matrix) % 3 == s:

                    @pl.when(t == n * per_matrix)
                    def _(n=n):
                        load_a(n)
                        if n + 1 < matrices:
                            fetch_a(n + 1)

            @pl.when(t < units)
            def _():
                multiply(t)

        return 0

    lax.fori_loop(0, (ticks + 3) // 3, three, 0)

    def last(u, _):
        for copy in out_copies(u):
            copy.wait()
        return 0

    lax.fori_loop(0, units, last, 0)


def sum_kernel(a, g):
    _, matrices, tokens, rows = a.shape
    columns = g.shape[3]
    units = matrices * columns // WIDTH
    dma = pltpu.SemaphoreType.DMA
    return pl.pallas_call(
        kernel,
        out_shape=jax.ShapeDtypeStruct((matrices, rows, columns), BF16),
        in_specs=[pl.BlockSpec(memory_space=pl.ANY)] * 2,
        out_specs=pl.BlockSpec(memory_space=pl.ANY),
        scratch_shapes=[
            pltpu.VMEM((tokens // TOKENS_AT_ONCE, TOKENS_AT_ONCE, rows), BF16),
            pltpu.VMEM((rows, tokens), BF16),
            pltpu.VMEM((2, tokens, WIDTH), BF16),
            pltpu.VMEM((SLOTS, 2, rows, LANES), BF16),
            pltpu.VMEM((SLOTS, 2, CHUNK[0], LANES), BF16),
            pltpu.VMEM((SLOTS, 2, CHUNK[1], LANES), BF16),
            pltpu.VMEM((SLOTS, 2, CHUNK[0], LANES), F32),
            pltpu.VMEM((SLOTS, 2, CHUNK[1], LANES), F32),
            *(pltpu.VMEM((SLOTS, 2, size, LANES), BF16) for size in CHUNK),
            *(pltpu.VMEM((units, 3, 2, size, LANES), BF16) for size in CHUNK),
            pltpu.VMEM((units, 2, rows, LANES), BF16),
            dma((tokens // TOKENS_AT_ONCE,)),
            dma((2,)),
            dma((units, 2)),
            dma((SLOTS, 3, 3, 2)),
            dma((units, 3, 3, 2)),
            dma((SLOTS, 3, 2, 2)),
            dma((units, 3, 2, 2)),
        ],
        compiler_params=pltpu.CompilerParams(
            collective_id=0, has_side_effects=True, vmem_limit_bytes=67_000_000
        ),
        name="sum_of_products",
    )(a, g)


def solution(mesh):
    return jax.shard_map(
        sum_kernel,
        mesh=mesh,
        in_specs=(P(("rep", "dp")), P(("rep", "dp"))),
        out_specs=P("rep"),
        check_vma=False,
    )
```

```python
import jax
import jax.numpy as jnp
from jax import lax
from jax.experimental import pallas as pl
from jax.experimental.pallas import tpu as pltpu
from jax.sharding import PartitionSpec as P

MESH = pl.DeviceIdType.MESH
F32, BF16 = jnp.float32, jnp.bfloat16
WIDTH = 256
LANES = 128
SLOTS = 6
SIDE = 4
STRIDE = (16, 4, 1)
CHUNK = (256, 64, 16)
TOKENS_AT_ONCE = 512
ROWS_AT_ONCE = 512

OFFSET = (1, 3, 5, 6, 7, 9, 10, 12, 13, 15, 17, 22, 27)
ORDER = (7, 2, 5, 12, 9, 1, 8, 0, 11, 3, 6, 4, 10)


def kernel(
    a_hbm, g_hbm, sums,
    a_in, a_t, g_in, tb0, tb1, tb2, tf1, tf2, mid0, mid1, mid2, got0, got1, got2,
    a_sem, g_sem, rs_send, rs_recv, ag_send, ag_recv,
):
    matrices, tokens, rows = a_hbm.shape[1], a_hbm.shape[2], a_hbm.shape[3]
    per_matrix = g_hbm.shape[3] // WIDTH
    units = matrices * per_matrix
    parts = tokens // TOKENS_AT_ONCE

    rep, me = lax.axis_index("rep"), lax.axis_index("dp")
    pos = tuple(lax.rem(me // s, SIDE) for s in STRIDE)

    def neighbour(axis, step):
        return me + (lax.rem(pos[axis] + step + SIDE, SIDE) - pos[axis]) * STRIDE[axis]

    right = tuple(neighbour(axis, 1) for axis in range(3))
    left = tuple(neighbour(axis, -1) for axis in range(3))

    tb, tf, mid, got = (tb0, tb1, tb2), (None, tf1, tf2), (mid0, mid1, mid2), (got0, got1, got2)

    def span(block, size):
        return pl.ds(pl.multiple_of(block * size, size), size)

    def put(src, dst, send, recv, device):
        return pltpu.make_async_remote_copy(
            src_ref=src, dst_ref=dst, send_sem=send, recv_sem=recv, device_id=(rep, device), device_id_type=MESH
        )

    def rs_put(src, u, c, p, kind, way):
        slot = lax.rem(u, SLOTS)
        device = (right, left)[way][(c + p) % 3]
        return put(
            src, got[p].at[u, kind, way], rs_send.at[slot, p, kind, way], rs_recv.at[u, p, kind, way], device
        )

    def rs_first(u, c, p):
        i, own = pos[(c + p) % 3], tb[p].at[lax.rem(u, SLOTS)]
        after, over, before = (span(lax.rem(i + k, SIDE), CHUNK[p]) for k in (1, 2, 3))
        return (
            rs_put(own.at[1, over], u, c, p, 0, 0),
            rs_put(own.at[0, over], u, c, p, 0, 1),
            rs_put(own.at[0, after], u, c, p, 1, 0),
            rs_put(own.at[1, before], u, c, p, 1, 1),
        )

    def rs_second(u, c, p):
        slot = lax.rem(u, SLOTS)
        return tuple(rs_put(mid[p].at[slot, way], u, c, p, 2, way) for way in (0, 1))

    def own_term(u, p, half, block):
        own = (tb[0] if p == 0 else tf[p])[lax.rem(u, SLOTS), half, span(block, CHUNK[p])]
        return own.astype(F32)

    def rs_middle(u, c, p):
        i, slot = pos[(c + p) % 3], lax.rem(u, SLOTS)
        copies = rs_first(u, c, p)
        for copy in copies[:2]:
            copy.wait_recv()
        for copy in copies:
            copy.wait_send()
        for way, half, step in ((0, 1, 1), (1, 0, 3)):
            total = own_term(u, p, half, lax.rem(i + step, SIDE)) + got[p][u, 0, way].astype(F32)
            mid[p][slot, way] = total.astype(BF16)

    def block_rows(c, p):
        first = 0
        for q in range(p):
            first = first + pos[(c + q) % 3] * CHUNK[q]
        return first

    def blk(c, p, step):
        first = block_rows(c, p) + lax.rem(pos[(c + p) % 3] + step, SIDE) * CHUNK[p]
        return pl.ds(pl.multiple_of(first, CHUNK[p]), CHUNK[p])

    def rs_end(u, c, p):
        i, slot = pos[(c + p) % 3], lax.rem(u, SLOTS)
        for copy in rs_first(u, c, p)[2:]:
            copy.wait_recv()
        for copy in rs_second(u, c, p):
            copy.wait_recv()
            copy.wait_send()
        for half in (0, 1):
            total = own_term(u, p, half, i) + got[p][u, 1, half].astype(F32) + got[p][u, 2, 1 - half].astype(F32)
            if p < 2:
                tf[p + 1][slot, half] = total
                tb[p + 1][slot, half] = total.astype(BF16)
            else:
                sums[u, half, blk(c, p, 0)] = total.astype(BF16)

    def ag_put(ref, u, c, p, step, way):
        slot = lax.rem(u, SLOTS)
        device = (right, left)[way][(c + p) % 3]
        return put(ref, ref, ag_send.at[slot, p, step, way], ag_recv.at[u, p, step, way], device)

    def ag_first(u, c, p):
        return tuple(ag_put(sums.at[u, :, blk(c, p, 0)], u, c, p, 0, way) for way in (0, 1))

    def ag_second(u, c, p):
        return (
            ag_put(sums.at[u, 0, blk(c, p, 3)], u, c, p, 1, 0),
            ag_put(sums.at[u, 1, blk(c, p, 1)], u, c, p, 1, 1),
        )

    def start(copies):
        for copy in copies:
            copy.start()

    def wait(copies):
        for copy in copies:
            copy.wait_recv()
            copy.wait_send()

    stages = (
        (lambda u, c: None, lambda u, c: start(rs_first(u, c, 0))),
        (lambda u, c: rs_middle(u, c, 0), lambda u, c: start(rs_second(u, c, 0))),
        (lambda u, c: rs_end(u, c, 0), lambda u, c: start(rs_first(u, c, 1))),
        (lambda u, c: rs_middle(u, c, 1), lambda u, c: start(rs_second(u, c, 1))),
        (lambda u, c: rs_end(u, c, 1), lambda u, c: start(rs_first(u, c, 2))),
        (lambda u, c: rs_middle(u, c, 2), lambda u, c: start(rs_second(u, c, 2))),
        (lambda u, c: rs_end(u, c, 2), lambda u, c: start(ag_first(u, c, 2))),
        (lambda u, c: wait(ag_first(u, c, 2)), lambda u, c: start(ag_second(u, c, 2))),
        (lambda u, c: wait(ag_second(u, c, 2)), lambda u, c: start(ag_first(u, c, 1))),
        (lambda u, c: wait(ag_first(u, c, 1)), lambda u, c: start(ag_second(u, c, 1))),
        (lambda u, c: wait(ag_second(u, c, 1)), lambda u, c: start(ag_first(u, c, 0))),
        (lambda u, c: wait(ag_first(u, c, 0)), lambda u, c: start(ag_second(u, c, 0))),
        (lambda u, c: wait(ag_second(u, c, 0)), lambda u, c: None),
    )

    def a_copy(n, part):
        return pltpu.make_async_copy(
            a_hbm.at[0, n, span(part, TOKENS_AT_ONCE)], a_in.at[part], a_sem.at[part]
        )

    def g_copy(u):
        n, j, slot = u // per_matrix, lax.rem(u, per_matrix), lax.rem(u, 2)
        return pltpu.make_async_copy(g_hbm.at[0, n, :, span(j, WIDTH)], g_in.at[slot], g_sem.at[slot])

    def load_a(n):
        def one(part, _):
            a_copy(n, part).wait()
            for column in range(0, rows, 256):
                block = a_in[part, :, column : column + 256]
                a_t[column : column + 256, span(part, TOKENS_AT_ONCE)] = block.T
            return 0

        lax.fori_loop(0, parts, one, 0)

    def fetch_a(n):
        def one(part, _):
            a_copy(n, part).start()
            return 0

        lax.fori_loop(0, parts, one, 0)

    def multiply(u):
        g_copy(u).wait()

        @pl.when(u + 1 < units)
        def _():
            g_copy(u + 1).start()

        def one(m, _):
            at = span(m, ROWS_AT_ONCE)
            term = jnp.dot(a_t[at, :], g_in[lax.rem(u, 2)], preferred_element_type=F32).astype(BF16)
            for half in (0, 1):
                tb0[lax.rem(u, SLOTS), half, at] = term[:, half * LANES : (half + 1) * LANES]
            return 0

        lax.fori_loop(0, rows // ROWS_AT_ONCE, one, 0)

    fetch_a(0)
    g_copy(0).start()

    barrier = pltpu.get_barrier_semaphore()
    for device in right + left:
        pl.semaphore_signal(barrier, inc=1, device_id=(rep, device), device_id_type=MESH)
    pl.semaphore_wait(barrier, 6)

    ticks = units + OFFSET[-1]

    def three(group, _):
        for s in range(3):
            t = group * 3 + s
            later = None

            def stage(k, which):
                u, c = t - OFFSET[k], (s - OFFSET[k]) % 3

                @pl.when(jnp.logical_and(u >= 0, u < units))
                def _():
                    stages[k][which](u, c)

            for k in ORDER:
                stage(k, 0)
                if later is not None:
                    stage(later, 1)
                later = k
            stage(later, 1)

            for n in range(matrices):
                if (n * per_matrix) % 3 == s:

                    @pl.when(t == n * per_matrix)
                    def _(n=n):
                        load_a(n)
                        if n + 1 < matrices:
                            fetch_a(n + 1)

            @pl.when(t < units)
            def _():
                multiply(t)

        return 0

    lax.fori_loop(0, (ticks + 3) // 3, three, 0)


def store_kernel(sums, out_hbm, sem):
    units = sums.shape[0]
    per_matrix = units // out_hbm.shape[0]

    def copy(u, half):
        n, j = u // per_matrix, lax.rem(u, per_matrix)
        at = pl.ds(pl.multiple_of(j * WIDTH + half * LANES, LANES), LANES)
        return pltpu.make_async_copy(sums.at[u, half], out_hbm.at[n, :, at], sem.at[u, half])

    def begin(u, _):
        for half in (0, 1):
            copy(u, half).start()
        return 0

    def end(u, _):
        for half in (0, 1):
            copy(u, half).wait()
        return 0

    lax.fori_loop(0, units, begin, 0)
    lax.fori_loop(0, units, end, 0)


def sum_kernel(a, g):
    _, matrices, tokens, rows = a.shape
    columns = g.shape[3]
    units = matrices * columns // WIDTH
    dma = pltpu.SemaphoreType.DMA
    sums = pl.pallas_call(
        kernel,
        out_shape=pltpu.VMEM((units, 2, rows, LANES), BF16),
        in_specs=[pl.BlockSpec(memory_space=pl.ANY)] * 2,
        out_specs=pl.BlockSpec(memory_space=pltpu.VMEM),
        scratch_shapes=[
            pltpu.VMEM((tokens // TOKENS_AT_ONCE, TOKENS_AT_ONCE, rows), BF16),
            pltpu.VMEM((rows, tokens), BF16),
            pltpu.VMEM((2, tokens, WIDTH), BF16),
            pltpu.VMEM((SLOTS, 2, rows, LANES), BF16),
            pltpu.VMEM((SLOTS, 2, CHUNK[0], LANES), BF16),
            pltpu.VMEM((SLOTS, 2, CHUNK[1], LANES), BF16),
            pltpu.VMEM((SLOTS, 2, CHUNK[0], LANES), F32),
            pltpu.VMEM((SLOTS, 2, CHUNK[1], LANES), F32),
            *(pltpu.VMEM((SLOTS, 2, size, LANES), BF16) for size in CHUNK),
            *(pltpu.VMEM((units, 3, 2, size, LANES), BF16) for size in CHUNK),
            dma((tokens // TOKENS_AT_ONCE,)),
            dma((2,)),
            dma((SLOTS, 3, 3, 2)),
            dma((units, 3, 3, 2)),
            dma((SLOTS, 3, 2, 2)),
            dma((units, 3, 2, 2)),
        ],
        compiler_params=pltpu.CompilerParams(
            collective_id=0, has_side_effects=True, vmem_limit_bytes=52_000_000
        ),
        name="sum_of_products",
    )(a, g)
    return pl.pallas_call(
        store_kernel,
        out_shape=jax.ShapeDtypeStruct((matrices, rows, columns), BF16),
        in_specs=[pl.BlockSpec(memory_space=pltpu.VMEM)],
        out_specs=pl.BlockSpec(memory_space=pl.ANY),
        scratch_shapes=[dma((units, 2))],
        compiler_params=pltpu.CompilerParams(vmem_limit_bytes=1 << 20),
        name="store",
    )(sums)


def solution(mesh):
    return jax.shard_map(
        sum_kernel,
        mesh=mesh,
        in_specs=(P(("rep", "dp")), P(("rep", "dp"))),
        out_specs=P("rep"),
        check_vma=False,
    )
```

```python
import functools

import jax
import jax.numpy as jnp
from jax import lax
from jax.experimental import pallas as pl
from jax.experimental.pallas import tpu as pltpu
from jax.sharding import PartitionSpec as P

MESH = pl.DeviceIdType.MESH
F32, BF16 = jnp.float32, jnp.bfloat16
WIDTH = 256
LANES = 128
SIDE = 4
STRIDE = (16, 4, 1)
CHUNK = (256, 64)
TOKENS_AT_ONCE = 512
TERM_SLOTS = 8
SUM_SLOTS = 12
DELTA = 1

OFFSET = (1, 3, 5, 7, 9, 10, 13, 15, 17, 29, 33)
ORDER = (10, 4, 3, 2, 7, 6, 1, 0, 8, 9, 5)
LOOPED = 27
DRAIN = (
    (9, 2), (3, 21), (5, 18), (1, 25), (2, 23), (6, 15), (9, 5), (3, 22), (4, 19), (7, 14), (6, 16), (9, 4), (4, 20),
    (4, 21), (6, 17), (3, 23), (4, 22), (2, 24), (2, 25), (6, 18), (9, 1), (9, 6), (5, 19), (8, 12), (7, 16), (5, 21),
    (7, 17), (5, 20), (3, 24), (7, 13), (7, 15), (4, 23), (7, 18), (3, 25), (10, 5), (9, 0), (9, 10), (8, 11),
    (5, 22), (8, 16), (9, 7), (4, 24), (4, 25), (6, 21), (6, 20), (9, 3), (5, 23), (6, 19), (9, 8), (8, 18), (5, 24),
    (6, 22), (5, 25), (7, 19), (10, 6), (8, 15), (8, 13), (8, 17), (7, 21), (6, 23), (7, 20), (6, 24), (10, 10),
    (6, 25), (7, 22), (9, 18), (8, 14), (8, 19), (7, 23), (7, 24), (10, 7), (8, 21), (8, 20), (7, 25), (9, 13),
    (9, 14), (8, 22), (8, 24), (8, 23), (10, 0), (9, 12), (9, 11), (8, 25), (9, 21), (9, 16), (9, 17), (10, 3),
    (9, 9), (9, 22), (9, 15), (9, 20), (10, 4), (10, 18), (9, 24), (10, 2), (9, 19), (10, 1), (10, 8), (9, 23),
    (10, 11), (9, 25), (10, 19), (10, 16), (10, 20), (10, 17), (10, 21), (10, 9), (10, 15), (10, 13), (10, 14),
    (10, 12), (10, 22), (10, 25), (10, 23), (10, 24),
)


def kernel(
    a_hbm, g_hbm, sums,
    a_in, a_t, g_in, tb0, tb1, tf1, mid0, mid1, got0, got1, parts_in,
    a_sem, g_sem, rs_send, rs_recv, ag_send, ag_recv,
):
    _, matrices, tokens, rows = a_hbm.shape
    per_matrix = g_hbm.shape[3] // WIDTH
    units = matrices * per_matrix
    pieces = tokens // TOKENS_AT_ONCE

    rep, me = lax.axis_index("rep"), lax.axis_index("dp")
    pos = tuple(lax.rem(me // s, SIDE) for s in STRIDE)

    def neighbour(axis, step):
        return me + (lax.rem(pos[axis] + step + SIDE, SIDE) - pos[axis]) * STRIDE[axis]

    right = tuple(neighbour(axis, 1) for axis in range(3))
    left = tuple(neighbour(axis, -1) for axis in range(3))

    tb, mid, got = (tb0, tb1), (mid0, mid1), (got0, got1)
    slots = (TERM_SLOTS, SUM_SLOTS)

    def axis_of(u, h, p):
        return (u[1] + h * DELTA + p) % 3

    def place(u, h, p):
        return pos[axis_of(u, h, p)]

    def device(u, h, p, way):
        return (right, left)[way][axis_of(u, h, p)]

    def slot(u, p):
        return lax.rem(u[0], slots[p])

    def turn(i, step):
        return lax.rem(i + step % SIDE, SIDE)

    def span(block, size, first=0):
        return pl.ds(pl.multiple_of(first + block * size, size), size)

    def put(src, dst, send, recv, u, h, p, way):
        return pltpu.make_async_remote_copy(
            src_ref=src,
            dst_ref=dst,
            send_sem=send,
            recv_sem=recv,
            device_id=(rep, device(u, h, p, way)),
            device_id_type=MESH,
        )

    def arrive(sem, like):
        pltpu.make_async_copy(like, like, sem).wait()

    def scatter_put(u, h, p, kind):
        if kind == 2:
            src = mid[p].at[slot(u, 1), h]
        else:
            step = 2 if kind == 0 else 1 - 2 * h
            src = tb[p].at[slot(u, p), h, span(turn(place(u, h, p), step), CHUNK[p])]
        send = rs_send.at[p, kind // 2, slot(u, 1)]
        recv = rs_recv.at[u[0], p, min(kind, 1)]
        return put(src, got[p].at[u[0], kind, h], send, recv, u, h, p, h if kind == 1 else 1 - h)

    def gather_ref(u, h, p, step):
        i = turn(place(u, h, p), step)
        if p == 2:
            return parts_in.at[u[0], h, i]
        first = place(u, h, 0) * CHUNK[0] if p == 1 else 0
        return sums.at[u[0], h, span(i, CHUNK[p], first)]

    def gather_put(u, h, p, kind):
        ref = gather_ref(u, h, p, (2 * h - 1) if kind == 2 else 0)
        send, recv = ag_send.at[u[0], p], ag_recv.at[u[0], p, min(kind, 1)]
        return put(ref, ref, send, recv, u, h, p, 1 - h if kind == 1 else h)

    def own_term(u, h, p, block):
        own = (tb0 if p == 0 else tf1)[slot(u, p), h, span(block, CHUNK[p])]
        return own.astype(F32)

    both = (0, 1)

    def scatter_send(u, p):
        for kind in (0, 1):
            for h in both:
                scatter_put(u, h, p, kind).start()

    def scatter_mid(u, p):
        arrive(rs_recv.at[u[0], p, 0], got[p].at[u[0], 0])
        for h in both:
            block = turn(place(u, h, p), 2 * h - 1)
            total = own_term(u, h, p, block) + got[p][u[0], 0, h].astype(F32)
            mid[p][slot(u, 1), h] = total.astype(BF16)

    def scatter_pass(u, p):
        for h in both:
            scatter_put(u, h, p, 2).start()

    def scatter_end(u, p):
        arrive(rs_recv.at[u[0], p, 1], got[p].at[u[0], 1:3])
        arrive(rs_send.at[p, 0, slot(u, 1)], got[p].at[u[0], 0:2])
        arrive(rs_send.at[p, 1, slot(u, 1)], got[p].at[u[0], 2])
        for h in both:
            i = place(u, h, p)
            total = own_term(u, h, p, i) + got[p][u[0], 1, h].astype(F32) + got[p][u[0], 2, h].astype(F32)
            if p == 0:
                tf1[slot(u, 1), h] = total
                tb1[slot(u, 1), h] = total.astype(BF16)
            else:
                parts_in[u[0], h, place(u, h, 2)] = total.astype(BF16)

    def gather_send(u, p):
        for kind in (0, 1):
            for h in both:
                gather_put(u, h, p, kind).start()

    def gather_pass(u, p):
        arrive(ag_recv.at[u[0], p, 0], got[min(p, 1)].at[u[0], 0])
        for h in both:
            gather_put(u, h, p, 2).start()

    def gather_end(u, p):
        arrive(ag_recv.at[u[0], p, 1], got[min(p, 1)].at[u[0], 1:3])
        arrive(ag_send.at[u[0], p], got[min(p, 1)].at[u[0]])

    def add_parts(u):
        gather_end(u, 2)
        for h in both:
            total = parts_in[u[0], h, 0].astype(F32)
            for i in range(1, SIDE):
                total = total + parts_in[u[0], h, i].astype(F32)
            first = place(u, h, 0) * CHUNK[0]
            sums[u[0], h, span(place(u, h, 1), CHUNK[1], first)] = total.astype(BF16)

    def gather_on(u):
        gather_end(u, 1)
        gather_send(u, 0)

    stages = (
        (lambda u: scatter_send(u, 0), None),
        (lambda u: scatter_mid(u, 0), lambda u: scatter_pass(u, 0)),
        (lambda u: scatter_end(u, 0), lambda u: scatter_send(u, 1)),
        (lambda u: scatter_mid(u, 1), lambda u: scatter_pass(u, 1)),
        (lambda u: scatter_end(u, 1), lambda u: gather_send(u, 2)),
        (lambda u: gather_pass(u, 2), None),
        (add_parts, lambda u: gather_send(u, 1)),
        (lambda u: gather_pass(u, 1), None),
        (gather_on, None),
        (lambda u: gather_pass(u, 0), None),
        (lambda u: gather_end(u, 0), None),
    )

    def each(first, last, f):
        def one(u, _):
            f(u)
            return 0

        lax.fori_loop(first, last, one, 0)

    def a_copy(n, piece):
        return pltpu.make_async_copy(a_hbm.at[0, n, span(piece, TOKENS_AT_ONCE)], a_in.at[piece], a_sem.at[piece])

    def g_copy(u):
        n, j, slot = u // per_matrix, lax.rem(u, per_matrix), lax.rem(u, 2)
        return pltpu.make_async_copy(g_hbm.at[0, n, :, span(j, WIDTH)], g_in.at[slot], g_sem.at[slot])

    def turn_a(piece, n):
        a_copy(n, piece).wait()
        for column in range(0, rows, 256):
            block = a_in[piece, :, column : column + 256]
            a_t[column : column + 256, span(piece, TOKENS_AT_ONCE)] = block.T

    def load_a(n):
        each(0, pieces, lambda piece: turn_a(piece, n))
        if n + 1 < matrices:
            each(0, pieces, lambda piece: a_copy(n + 1, piece).start())

    def multiply(u):
        g_copy(u).wait()

        @pl.when(u + 1 < units)
        def _():
            g_copy(u + 1).start()

        term = jnp.dot(a_t[...], g_in[lax.rem(u, 2)], preferred_element_type=F32).astype(BF16)
        for h in both:
            tb0[lax.rem(u, TERM_SLOTS), h] = term[:, h * LANES : (h + 1) * LANES]

    each(0, pieces, lambda piece: a_copy(0, piece).start())
    g_copy(0).start()
    barrier = pltpu.get_barrier_semaphore()
    for other in right + left:
        pl.semaphore_signal(barrier, inc=1, device_id=(rep, other), device_id_type=MESH)
    load_a(0)
    multiply(jnp.int32(0))
    pl.semaphore_wait(barrier, 6)

    def three(group, _):
        for s in range(3):
            t = group * 3 + s + 1
            late = None
            for k in ORDER:
                number, colour = t - OFFSET[k], (s + 1 - OFFSET[k]) % 3
                now, then = stages[k]
                due = jnp.logical_and(number >= 0, number < units)

                @pl.when(due)
                def _():
                    now((number, colour))

                if late is not None:
                    pl.when(late[0])(late[1])
                late = None if then is None else (due, functools.partial(then, (number, colour)))
            if late is not None:
                pl.when(late[0])(late[1])

            for n in range(1, matrices):
                if (n * per_matrix - 1) % 3 == s:

                    @pl.when(t == n * per_matrix)
                    def _():
                        load_a(n)

            @pl.when(t < units)
            def _():
                multiply(t)

        return 0

    lax.fori_loop(0, LOOPED // 3, three, 0)

    late = None
    for k, u in DRAIN:
        now, then = stages[k]
        now((jnp.int32(u), u % 3))
        if late is not None:
            late()
        late = None if then is None else functools.partial(then, (jnp.int32(u), u % 3))


def store_kernel(sums, out_hbm, sem):
    units = sums.shape[0]
    per_matrix = units // out_hbm.shape[0]

    def copy(u, half):
        n, j = u // per_matrix, lax.rem(u, per_matrix)
        at = pl.ds(pl.multiple_of(j * WIDTH + half * LANES, LANES), LANES)
        return pltpu.make_async_copy(sums.at[u, half], out_hbm.at[n, :, at], sem.at[u, half])

    def begin(u, _):
        for half in (0, 1):
            copy(u, half).start()
        return 0

    def end(u, _):
        for half in (0, 1):
            copy(u, half).wait()
        return 0

    lax.fori_loop(0, units, begin, 0)
    lax.fori_loop(0, units, end, 0)


def sum_products(a, g):
    _, matrices, tokens, rows = a.shape
    columns = g.shape[3]
    units = matrices * columns // WIDTH
    dma = pltpu.SemaphoreType.DMA
    sums = pl.pallas_call(
        kernel,
        out_shape=pltpu.VMEM((units, 2, rows, LANES), BF16),
        in_specs=[pl.BlockSpec(memory_space=pl.ANY)] * 2,
        out_specs=pl.BlockSpec(memory_space=pltpu.VMEM),
        scratch_shapes=[
            pltpu.VMEM((tokens // TOKENS_AT_ONCE, TOKENS_AT_ONCE, rows), BF16),
            pltpu.VMEM((rows, tokens), BF16),
            pltpu.VMEM((2, tokens, WIDTH), BF16),
            pltpu.VMEM((TERM_SLOTS, 2, rows, LANES), BF16),
            pltpu.VMEM((SUM_SLOTS, 2, CHUNK[0], LANES), BF16),
            pltpu.VMEM((SUM_SLOTS, 2, CHUNK[0], LANES), F32),
            *(pltpu.VMEM((SUM_SLOTS, 2, size, LANES), BF16) for size in CHUNK),
            *(pltpu.VMEM((units, 3, 2, size, LANES), BF16) for size in CHUNK),
            pltpu.VMEM((units, 2, SIDE, CHUNK[1], LANES), BF16),
            dma((tokens // TOKENS_AT_ONCE,)),
            dma((2,)),
            dma((2, 2, SUM_SLOTS)),
            dma((units, 2, 2)),
            dma((units, 3)),
            dma((units, 3, 2)),
        ],
        compiler_params=pltpu.CompilerParams(
            collective_id=0, has_side_effects=True, vmem_limit_bytes=53_000_000
        ),
        name="sum_of_products",
    )(a, g)
    return pl.pallas_call(
        store_kernel,
        out_shape=jax.ShapeDtypeStruct((matrices, rows, columns), BF16),
        in_specs=[pl.BlockSpec(memory_space=pltpu.VMEM)],
        out_specs=pl.BlockSpec(memory_space=pl.ANY),
        scratch_shapes=[dma((units, 2))],
        compiler_params=pltpu.CompilerParams(vmem_limit_bytes=1 << 20),
        name="store",
    )(sums)


def solution(mesh):
    return jax.shard_map(
        sum_products,
        mesh=mesh,
        in_specs=(P(("rep", "dp")), P(("rep", "dp"))),
        out_specs=P("rep"),
        check_vma=False,
    )
```
